32 devices in a mesh: cells: 8 (over y, x, core), genes: 4 (over z).
Axes of the slice: x: 2, y: 2, z: 4, core: 2. Of those that a mesh axis runs over, the one named last changes fastest.
Arguments:
- counts: int32 [8192, 4096], P('cells', 'genes'), may hold values from 0 to 26, as said below
- library: int32 [8192], P('cells'), may hold values from 2000 to 19999
Outputs:
- adjacency: float32 [4096, 4096], P('cells', 'genes')
- connectivity: float32 [4096], P('cells')
The draws below stay inside these ranges and needn't reach their ends.
Inputs may be any that keep to these rules, and one draw needn't show every extreme that they name: Non-negative integer counts.
All inputs are finite; a program needn't handle non-finite values.
Results may differ from the reference program's by a relative error of at most 0.006.
Values may be sent and summed in bfloat16 or wider, within the bound.
A program may use at most 128 MiB of HBM per device.

```python
import jax
import jax.numpy as jnp
from jax import lax

G = 4096
CELLS_DEV = 1024
CELLS = 8192
N_CELLS = 8


module_count = 32


def draw_counts(key, part):
    module_ids = jax.random.randint(jax.random.fold_in(key, 11), (G,), 0, module_count)
    levels = jax.random.randint(jax.random.fold_in(key, 12), (CELLS, module_count), 0, 8)
    gains = jax.random.randint(jax.random.fold_in(key, 13), (G,), 0, 4)
    noise = jax.random.randint(jax.random.fold_in(key, 14), (CELLS, G), 0, 6)
    present = jax.random.randint(jax.random.fold_in(key, 15), (CELLS, G), 0, 3)
    shared = jnp.take(levels, module_ids, axis=1)
    values = noise + gains[None, :] * shared
    return jnp.where(present > 0, values, 0).astype(jnp.int32)


def place_ends(values, rng, low, high):
    longest = values.shape.index(max(values.shape))
    spots = []
    for shift in (0, 1):
        where = [jax.random.randint(jax.random.fold_in(rng, axis), (), 0, length) for axis, length in enumerate(values.shape)]
        where[longest] = (where[longest] + shift) % values.shape[longest]
        spots.append(tuple(where))
    return values.at[spots[0]].set(low).at[spots[1]].set(high)


def setup_inputs(seed: int = 0) -> dict:
    splits = jax.random.split(jax.random.key(seed), 3)
    return {
        "counts": draw_counts(jax.random.fold_in(splits[2], 71), 0),
        "library": place_ends(jax.random.randint(splits[1], (CELLS,), 2000, 20000), jax.random.fold_in(splits[1], 1), 2000, 19999).astype(jnp.int32),
    }


def normalize(counts, library):
    factor = 10000.0 / library.astype(jnp.float32)
    return jnp.log1p(counts.astype(jnp.float32) * factor[:, None]).astype(jnp.bfloat16)

def reference(counts, library):
    count_blocks = counts.reshape(N_CELLS, CELLS_DEV, G)
    library_blocks = library.reshape(N_CELLS, CELLS_DEV)

    def accumulate(carry, inputs):
        gram, sums, squares = carry
        expressed = normalize(inputs[0], inputs[1]).astype(jnp.float32)
        gram = gram + jnp.dot(expressed.T, expressed, precision=lax.Precision.HIGHEST, preferred_element_type=jnp.float32)
        sums = sums + lax.optimization_barrier(jnp.sum(expressed, axis=0))
        squares = squares + lax.optimization_barrier(jnp.sum(expressed * expressed, axis=0))
        return ((gram, sums, squares), None)
    start = (jnp.zeros((G, G), jnp.float32), jnp.zeros((G,), jnp.float32), jnp.zeros((G,), jnp.float32))
    (gram, sums, squares), unused = lax.scan(accumulate, start, (count_blocks, library_blocks))
    total_cells = float(CELLS)
    means = sums / total_cells
    variances = squares / total_cells - means * means
    scales = lax.rsqrt(variances + 1e-05)
    correlation = (gram / total_cells - means[:, None] * means[None, :]) * scales[:, None] * scales[None, :]
    powered = correlation ** 6
    diagonal = jnp.arange(G)[:, None] == jnp.arange(G)[None, :]
    adjacency = jnp.where(diagonal, jnp.float32(0.0), powered)
    connectivity = lax.optimization_barrier(jnp.sum(adjacency, axis=1))
    return (adjacency, connectivity)
```

```python
import jax
import jax.numpy as jnp
from jax import lax
from jax.sharding import PartitionSpec as P

CHUNKS = 4
DEPTH = 3


def normalize(counts, library):
    factor = 10000.0 / library.astype(jnp.float32)
    return jnp.log1p(counts.astype(jnp.float32) * factor[:, None]).astype(jnp.bfloat16)


def shards(counts, library):
    own_block = normalize(counts, library)
    cells, col_width = own_block.shape
    cell_groups = lax.axis_size("cells")
    gene_groups = lax.axis_size("genes")
    row_width = col_width * gene_groups // cell_groups
    owners = col_width // row_width
    part = row_width // CHUNKS
    total_cells = float(cells * cell_groups)
    me = lax.axis_index("genes")
    ring = [(i, (i + 1) % gene_groups) for i in range(gene_groups)]

    split = own_block.reshape(cells, owners, CHUNKS, part)
    flights = []
    blocks = []
    for q in range(CHUNKS):
        held = split[:, :, q, :].reshape(cells, owners * part)
        mine = [held]
        for step in range(gene_groups - 1):
            if len(flights) >= DEPTH:
                held, flights[-DEPTH] = lax.optimization_barrier((held, flights[-DEPTH]))
            held = lax.ppermute(held, "genes", ring)
            flights.append(held)
            mine.append(held)
        blocks.append(mine)

    widened = own_block.astype(jnp.float32)
    sums = jnp.stack([jnp.sum(widened, axis=0), jnp.sum(widened * widened, axis=0)])
    sums = lax.psum(sums, "cells")
    all_sums = lax.all_gather(sums, "genes", axis=1, tiled=True)

    pieces = []
    for q in range(CHUNKS):
        tiles = jnp.zeros((gene_groups, owners * part, col_width), jnp.float32)
        for step in range(gene_groups):
            source = lax.rem(me - step + gene_groups, gene_groups)
            tile = lax.dot_general(
                blocks[q][step], own_block, (((0,), (0,)), ((), ())), preferred_element_type=jnp.float32
            )
            tiles = lax.dynamic_update_slice(tiles, tile[None], (source, 0, 0))
        tiles = tiles.reshape(cell_groups * part, col_width)
        pieces.append(lax.psum_scatter(tiles, "cells", scatter_dimension=0, tiled=True))
    gram_tile = jnp.concatenate(pieces, axis=0)

    means = all_sums[0] / total_cells
    variances = all_sums[1] / total_cells - means * means
    scales = lax.rsqrt(variances + 1e-05)
    row_first = lax.axis_index("cells") * row_width
    col_first = me * col_width
    row_means = lax.dynamic_slice_in_dim(means, row_first, row_width, 0)
    col_means = lax.dynamic_slice_in_dim(means, col_first, col_width, 0)
    row_scales = lax.dynamic_slice_in_dim(scales, row_first, row_width, 0)
    col_scales = lax.dynamic_slice_in_dim(scales, col_first, col_width, 0)
    correlation = (
        (gram_tile / total_cells - row_means[:, None] * col_means[None, :])
        * row_scales[:, None]
        * col_scales[None, :]
    )
    powered = correlation**6
    row_index = row_first + jnp.arange(row_width, dtype=jnp.int32)[:, None]
    col_index = col_first + jnp.arange(col_width, dtype=jnp.int32)[None, :]
    adjacency = jnp.where(row_index == col_index, jnp.float32(0.0), powered)
    connectivity = lax.psum(jnp.sum(adjacency, axis=1), "genes")
    return (adjacency, connectivity)


def solution(mesh):
    return jax.shard_map(
        shards,
        mesh=mesh,
        in_specs=(P("cells", "genes"), P("cells")),
        out_specs=(P("cells", "genes"), P("cells")),
        check_vma=False,
    )
```

```python
import functools

import jax
import jax.numpy as jnp
from jax import lax
from jax.experimental import pallas as pl
from jax.experimental.pallas import tpu as pltpu
from jax.sharding import PartitionSpec as P

CHUNKS = 4
TILE = 256


def bit(value, index):
    return (value // (1 << index)) % 2


def flip(value, index):
    return value + (1 << index) * (1 - 2 * bit(value, index))


def network(cell_groups, gene_groups, owners, xq_ref, own_ref, sums_ref, out_ref, stats_ref,
            held, partial, landed, totals, sums_in,
            ring_send, ring_recv, cut_send, cut_recv, fly_send, fly_recv, stat_send, stat_recv):
    chunks, rows, cells = xq_ref.shape
    part = rows // owners
    cols = own_ref.shape[1]
    half = cols // 2
    c = lax.axis_index("cells")
    g = lax.axis_index("genes")
    right = lax.rem(g + 1, gene_groups)
    left = lax.rem(g + gene_groups - 1, gene_groups)
    bits = cell_groups.bit_length() - 1
    hops = gene_groups - 1
    orders = (tuple(range(bits)), (0,) + tuple(range(bits - 1, 0, -1)))

    barrier = pltpu.get_barrier_semaphore()
    for target in [(c, left), (c, right)] + [(flip(c, b), g) for b in range(bits)]:
        pl.semaphore_signal(barrier, inc=1, device_id=target, device_id_type=pl.DeviceIdType.MESH)
    pl.semaphore_wait(barrier, 2 + bits)

    def ring(q, hop, piece):
        span = pl.ds(piece * (rows // 2), rows // 2)
        source = xq_ref.at[q, span] if hop == 0 else held.at[q, hop - 1, span]
        return pltpu.make_async_remote_copy(
            src_ref=source, dst_ref=held.at[q, hop, span],
            send_sem=ring_send.at[q, hop, piece], recv_sem=ring_recv.at[q, hop, piece],
            device_id=(c, right), device_id_type=pl.DeviceIdType.MESH)

    def cut(q, side, stage):
        count = cell_groups >> (stage + 1)
        return pltpu.make_async_remote_copy(
            src_ref=partial.at[q, side, pl.ds(count, count)],
            dst_ref=landed.at[q, side, pl.ds(count, count)],
            send_sem=cut_send.at[q, side, stage], recv_sem=cut_recv.at[q, side, stage],
            device_id=(flip(c, orders[side][stage]), g), device_id_type=pl.DeviceIdType.MESH)

    def fly(stage):
        return pltpu.make_async_remote_copy(
            src_ref=totals.at[stage], dst_ref=sums_in.at[stage],
            send_sem=fly_send.at[stage], recv_sem=fly_recv.at[stage],
            device_id=(flip(c, stage), g), device_id_type=pl.DeviceIdType.MESH)

    def spread(hop):
        source = totals.at[bits] if hop == 0 else stats_ref.at[hop]
        return pltpu.make_async_remote_copy(
            src_ref=source, dst_ref=stats_ref.at[hop + 1],
            send_sem=stat_send.at[hop], recv_sem=stat_recv.at[hop],
            device_id=(c, right), device_id_type=pl.DeviceIdType.MESH)

    def place(owner, side):
        total = 0
        for position, b in enumerate(orders[side]):
            total = total + ((bit(owner, b) + bit(c, b)) % 2) * (1 << (bits - 1 - position))
        return total

    def multiply(q, step):
        source = lax.rem(g - step + gene_groups, gene_groups)
        block = xq_ref.at[q] if step == 0 else held.at[q, step - 1]
        for side in range(2):
            spots = [place(source * owners + o, side) for o in range(owners)]

            @pl.loop(0, half // TILE)
            def _(t):
                start = pl.multiple_of(t * TILE, TILE)
                columns = pl.ds(pl.multiple_of(side * half + start, TILE), TILE)
                tile = jnp.dot(block[...], own_ref[:, columns], preferred_element_type=jnp.float32)
                for o in range(owners):
                    partial[q, side, spots[o], :, pl.ds(start, TILE)] = tile[o * part:(o + 1) * part]

    def launch(q, stage):
        for side in range(2):
            cut(q, side, stage).start()

    def absorb(q, stage):
        count = cell_groups >> (stage + 1)
        for side in range(2):
            cut(q, side, stage).wait_recv()
            if count > 1:
                @pl.loop(0, count)
                def _(i):
                    partial[q, side, i] = partial[q, side, i] + landed[q, side, i + count]
            else:
                out_ref[pl.ds(q * part, part), side * half:(side + 1) * half] = (
                    partial[q, side, 0] + landed[q, side, 1])

    for piece in range(2):
        ring(0, 0, piece).start()
    totals[0] = sums_ref[...]
    for stage in range(bits):
        fly(stage).start()
        fly(stage).wait_recv()
        totals[stage + 1] = totals[stage] + sums_in[stage]
    stats_ref[0] = totals[bits]

    turns = [[s for s in range(bits) if s * hops // bits == h] for h in range(hops)]

    @pl.loop(0, chunks)
    def _(q):
        multiply(q, 0)
        for hop in range(hops):
            for piece in range(2):
                ring(q, hop, piece).wait_recv()
                if hop < hops - 1:
                    ring(q, hop + 1, piece).start()
            if hop == max(hops - 2, 0):
                @pl.when(q < chunks - 1)
                def _():
                    for piece in range(2):
                        ring(q + 1, 0, piece).start()

            @pl.when(q > 0)
            def _():
                for stage in turns[hop]:
                    absorb(q - 1, stage)
                    if stage + 1 < bits:
                        launch(q - 1, stage + 1)
            multiply(q, hop + 1)
        launch(q, 0)

    last = chunks - 1
    spread(0).start()
    for stage in range(bits):
        absorb(last, stage)
        if stage + 1 < bits:
            launch(last, stage + 1)
        if stage < hops:
            spread(stage).wait_recv()
            if stage + 1 < hops:
                spread(stage + 1).start()
    for hop in range(bits, hops):
        spread(hop).wait_recv()
        if hop + 1 < hops:
            spread(hop + 1).start()
    for hop in range(hops):
        spread(hop).wait_send()
    for stage in range(bits):
        fly(stage).wait_send()

    @pl.loop(0, chunks)
    def _(q):
        for hop in range(hops):
            for piece in range(2):
                ring(q, hop, piece).wait_send()
        for side in range(2):
            for stage in range(bits):
                cut(q, side, stage).wait_send()


def normalize(counts, library):
    factor = 10000.0 / library.astype(jnp.float32)
    return jnp.log1p(counts.astype(jnp.float32) * factor[:, None]).astype(jnp.bfloat16)


def shards(counts, library):
    own_block = normalize(counts, library)
    cells, col_width = own_block.shape
    cell_groups = lax.axis_size("cells")
    gene_groups = lax.axis_size("genes")
    row_width = col_width * gene_groups // cell_groups
    owners = col_width // row_width
    part = row_width // CHUNKS
    total_cells = float(cells * cell_groups)
    me = lax.axis_index("genes")

    transposed = own_block.T.reshape(owners, CHUNKS, part, cells)
    ordered = jnp.transpose(transposed, (1, 0, 2, 3)).reshape(CHUNKS, owners * part, cells)
    widened = own_block.astype(jnp.float32)
    sums = jnp.stack([jnp.sum(widened, axis=0), jnp.sum(widened * widened, axis=0)])
    sums = jnp.concatenate([sums, jnp.zeros((6, col_width), jnp.float32)], axis=0)
    bits = cell_groups.bit_length() - 1
    hops = gene_groups - 1
    vmem = pl.BlockSpec(memory_space=pltpu.VMEM)
    dma = pltpu.SemaphoreType.DMA
    gram_tile, stats = pl.pallas_call(
        functools.partial(network, cell_groups, gene_groups, owners),
        out_shape=(
            jax.ShapeDtypeStruct((row_width, col_width), jnp.float32),
            jax.ShapeDtypeStruct((gene_groups, 8, col_width), jnp.float32),
        ),
        in_specs=[vmem] * 3,
        out_specs=(vmem, vmem),
        scratch_shapes=[
            pltpu.VMEM((CHUNKS, hops, owners * part, cells), jnp.bfloat16),
            pltpu.VMEM((CHUNKS, 2, cell_groups, part, col_width // 2), jnp.float32),
            pltpu.VMEM((CHUNKS, 2, cell_groups, part, col_width // 2), jnp.float32),
            pltpu.VMEM((bits + 1, 8, col_width), jnp.float32),
            pltpu.VMEM((bits, 8, col_width), jnp.float32),
            dma((CHUNKS, hops, 2)), dma((CHUNKS, hops, 2)),
            dma((CHUNKS, 2, bits)), dma((CHUNKS, 2, bits)),
            dma((bits,)), dma((bits,)),
            dma((hops,)), dma((hops,)),
        ],
        compiler_params=pltpu.CompilerParams(
            collective_id=0, has_side_effects=True, vmem_limit_bytes=60 * 1024 * 1024),
    )(ordered, own_block, sums)
    order = lax.rem(me - jnp.arange(gene_groups) + gene_groups, gene_groups)
    all_sums = jnp.transpose(jnp.take(stats[:, :2], order, axis=0), (1, 0, 2)).reshape(2, -1)

    means = all_sums[0] / total_cells
    variances = all_sums[1] / total_cells - means * means
    scales = lax.rsqrt(variances + 1e-05)
    row_first = lax.axis_index("cells") * row_width
    col_first = me * col_width
    row_means = lax.dynamic_slice_in_dim(means, row_first, row_width, 0)
    col_means = lax.dynamic_slice_in_dim(means, col_first, col_width, 0)
    row_scales = lax.dynamic_slice_in_dim(scales, row_first, row_width, 0)
    col_scales = lax.dynamic_slice_in_dim(scales, col_first, col_width, 0)
    correlation = (
        (gram_tile / total_cells - row_means[:, None] * col_means[None, :])
        * row_scales[:, None]
        * col_scales[None, :]
    )
    powered = correlation**6
    row_index = row_first + jnp.arange(row_width, dtype=jnp.int32)[:, None]
    col_index = col_first + jnp.arange(col_width, dtype=jnp.int32)[None, :]
    adjacency = jnp.where(row_index == col_index, jnp.float32(0.0), powered)
    connectivity = lax.psum(jnp.sum(adjacency, axis=1), "genes")
    return (adjacency, connectivity)


def solution(mesh):
    return jax.shard_map(
        shards,
        mesh=mesh,
        in_specs=(P("cells", "genes"), P("cells")),
        out_specs=(P("cells", "genes"), P("cells")),
        check_vma=False,
    )
```

```python
import functools

import jax
import jax.numpy as jnp
from jax import lax
from jax.experimental import pallas as pl
from jax.experimental.pallas import tpu as pltpu
from jax.sharding import PartitionSpec as P

CHUNKS = 8
TILE = 512


def bit(value, index):
    return (value // (1 << index)) % 2


def flip(value, index):
    return value + (1 << index) * (1 - 2 * bit(value, index))


def network(cell_groups, gene_groups, xq_ref, own_ref, sums_ref, out_ref, stats_ref,
            held, partial, landed, totals, sums_in,
            ring_send, ring_recv, cut_send, cut_recv, fly_send, fly_recv, stat_send, stat_recv):
    owners, chunks, part, cells = xq_ref.shape
    rows = owners * part
    cols = own_ref.shape[1]
    half = cols // 2
    c = lax.axis_index("cells")
    g = lax.axis_index("genes")
    right = lax.rem(g + 1, gene_groups)
    left = lax.rem(g + gene_groups - 1, gene_groups)
    bits = cell_groups.bit_length() - 1
    hops = gene_groups - 1
    orders = (tuple(range(bits)), (0,) + tuple(range(bits - 1, 0, -1)))

    barrier = pltpu.get_barrier_semaphore()
    for target in [(c, left), (c, right)] + [(flip(c, b), g) for b in range(bits)]:
        pl.semaphore_signal(barrier, inc=1, device_id=target, device_id_type=pl.DeviceIdType.MESH)
    pl.semaphore_wait(barrier, 2 + bits)

    def ring(q, hop, piece):
        span = pl.ds(piece * (owners // 2), owners // 2)
        source = xq_ref.at[span, q] if hop == 0 else held.at[q, hop - 1, span]
        return pltpu.make_async_remote_copy(
            src_ref=source, dst_ref=held.at[q, hop, span],
            send_sem=ring_send.at[q, hop, piece], recv_sem=ring_recv.at[q, hop, piece],
            device_id=(c, right), device_id_type=pl.DeviceIdType.MESH)

    def cut(q, side, stage):
        count = cell_groups >> (stage + 1)
        return pltpu.make_async_remote_copy(
            src_ref=partial.at[q, side, pl.ds(count, count)],
            dst_ref=landed.at[q, side, pl.ds(count, count)],
            send_sem=cut_send.at[q, side, stage], recv_sem=cut_recv.at[q, side, stage],
            device_id=(flip(c, orders[side][stage]), g), device_id_type=pl.DeviceIdType.MESH)

    def fly(stage):
        return pltpu.make_async_remote_copy(
            src_ref=totals.at[stage], dst_ref=sums_in.at[stage],
            send_sem=fly_send.at[stage], recv_sem=fly_recv.at[stage],
            device_id=(flip(c, stage), g), device_id_type=pl.DeviceIdType.MESH)

    def spread(hop):
        source = totals.at[bits] if hop == 0 else stats_ref.at[hop]
        return pltpu.make_async_remote_copy(
            src_ref=source, dst_ref=stats_ref.at[hop + 1],
            send_sem=stat_send.at[hop], recv_sem=stat_recv.at[hop],
            device_id=(c, right), device_id_type=pl.DeviceIdType.MESH)

    def place(owner, side):
        total = 0
        for position, b in enumerate(orders[side]):
            total = total + ((bit(owner, b) + bit(c, b)) % 2) * (1 << (bits - 1 - position))
        return total

    def multiply(q, step):
        source = lax.rem(g - step + gene_groups, gene_groups)
        block = xq_ref.at[:, q] if step == 0 else held.at[q, step - 1]
        for side in range(2):
            spots = [place(source * owners + o, side) for o in range(owners)]

            @pl.loop(0, half // TILE)
            def _(t):
                start = pl.multiple_of(t * TILE, TILE)
                columns = pl.ds(pl.multiple_of(side * half + start, TILE), TILE)
                tile = jnp.dot(block[...].reshape(rows, cells), own_ref[:, columns], preferred_element_type=jnp.float32)
                for o in range(owners):
                    partial[q, side, spots[o], :, pl.ds(start, TILE)] = tile[o * part:(o + 1) * part]

    def launch(q, stage):
        for side in range(2):
            cut(q, side, stage).start()

    def absorb(q, stage):
        count = cell_groups >> (stage + 1)
        for side in range(2):
            cut(q, side, stage).wait_recv()
            if count > 1:
                @pl.loop(0, count)
                def _(i):
                    partial[q, side, i] = partial[q, side, i] + landed[q, side, i + count]
            else:
                out_ref[pl.ds(q * part, part), side * half:(side + 1) * half] = (
                    partial[q, side, 0] + landed[q, side, 1])

    for piece in range(2):
        ring(0, 0, piece).start()
    totals[0] = sums_ref[...]
    for stage in range(bits):
        fly(stage).start()
        fly(stage).wait_recv()
        totals[stage + 1] = totals[stage] + sums_in[stage]
    stats_ref[0] = totals[bits]

    turns = [[s for s in range(bits) if s * hops // bits == h] for h in range(hops)]

    @pl.loop(0, chunks)
    def _(q):
        multiply(q, 0)
        for hop in range(hops):
            for piece in range(2):
                ring(q, hop, piece).wait_recv()
                if hop < hops - 1:
                    ring(q, hop + 1, piece).start()
            if hop == max(hops - 2, 0):
                @pl.when(q < chunks - 1)
                def _():
                    for piece in range(2):
                        ring(q + 1, 0, piece).start()

            @pl.when(q > 0)
            def _():
                for stage in turns[hop]:
                    absorb(q - 1, stage)
                    if stage + 1 < bits:
                        launch(q - 1, stage + 1)
            multiply(q, hop + 1)
        launch(q, 0)

    last = chunks - 1
    spread(0).start()
    for stage in range(bits):
        absorb(last, stage)
        if stage + 1 < bits:
            launch(last, stage + 1)
        if stage < hops:
            spread(stage).wait_recv()
            if stage + 1 < hops:
                spread(stage + 1).start()
    for hop in range(bits, hops):
        spread(hop).wait_recv()
        if hop + 1 < hops:
            spread(hop + 1).start()
    for hop in range(hops):
        spread(hop).wait_send()
    for stage in range(bits):
        fly(stage).wait_send()

    @pl.loop(0, chunks)
    def _(q):
        for hop in range(hops):
            for piece in range(2):
                ring(q, hop, piece).wait_send()
        for side in range(2):
            for stage in range(bits):
                cut(q, side, stage).wait_send()


def normalize(counts, library):
    factor = 10000.0 / library.astype(jnp.float32)
    return jnp.log1p(counts.astype(jnp.float32) * factor[:, None]).astype(jnp.bfloat16)


def shards(counts, library):
    own_block = normalize(counts, library)
    cells, col_width = own_block.shape
    cell_groups = lax.axis_size("cells")
    gene_groups = lax.axis_size("genes")
    row_width = col_width * gene_groups // cell_groups
    owners = col_width // row_width
    total_cells = float(cells * cell_groups)
    me = lax.axis_index("genes")

    chunks = min(CHUNKS, row_width // 16)
    part = row_width // chunks
    ordered = own_block.T.reshape(owners, chunks, part, cells)
    widened = own_block.astype(jnp.float32)
    sums = jnp.stack([jnp.sum(widened, axis=0), jnp.sum(widened * widened, axis=0)])
    sums = jnp.concatenate([sums, jnp.zeros((6, col_width), jnp.float32)], axis=0)
    bits = cell_groups.bit_length() - 1
    hops = gene_groups - 1
    vmem = pl.BlockSpec(memory_space=pltpu.VMEM)
    dma = pltpu.SemaphoreType.DMA
    gram_tile, stats = pl.pallas_call(
        functools.partial(network, cell_groups, gene_groups),
        out_shape=(
            jax.ShapeDtypeStruct((row_width, col_width), jnp.float32),
            jax.ShapeDtypeStruct((gene_groups, 8, col_width), jnp.float32),
        ),
        in_specs=[vmem] * 3,
        out_specs=(vmem, vmem),
        scratch_shapes=[
            pltpu.VMEM((chunks, hops, owners, part, cells), jnp.bfloat16),
            pltpu.VMEM((chunks, 2, cell_groups, part, col_width // 2), jnp.float32),
            pltpu.VMEM((chunks, 2, cell_groups, part, col_width // 2), jnp.float32),
            pltpu.VMEM((bits + 1, 8, col_width), jnp.float32),
            pltpu.VMEM((bits, 8, col_width), jnp.float32),
            dma((chunks, hops, 2)), dma((chunks, hops, 2)),
            dma((chunks, 2, bits)), dma((chunks, 2, bits)),
            dma((bits,)), dma((bits,)),
            dma((hops,)), dma((hops,)),
        ],
        compiler_params=pltpu.CompilerParams(
            collective_id=0, has_side_effects=True, vmem_limit_bytes=60 * 1024 * 1024),
    )(ordered, own_block, sums)
    order = lax.rem(me - jnp.arange(gene_groups) + gene_groups, gene_groups)
    all_sums = jnp.transpose(jnp.take(stats[:, :2], order, axis=0), (1, 0, 2)).reshape(2, -1)

    means = all_sums[0] / total_cells
    variances = all_sums[1] / total_cells - means * means
    scales = lax.rsqrt(variances + 1e-05)
    row_first = lax.axis_index("cells") * row_width
    col_first = me * col_width
    row_means = lax.dynamic_slice_in_dim(means, row_first, row_width, 0)
    col_means = lax.dynamic_slice_in_dim(means, col_first, col_width, 0)
    row_scales = lax.dynamic_slice_in_dim(scales, row_first, row_width, 0)
    col_scales = lax.dynamic_slice_in_dim(scales, col_first, col_width, 0)
    correlation = (
        (gram_tile / total_cells - row_means[:, None] * col_means[None, :])
        * row_scales[:, None]
        * col_scales[None, :]
    )
    powered = correlation**6
    row_index = row_first + jnp.arange(row_width, dtype=jnp.int32)[:, None]
    col_index = col_first + jnp.arange(col_width, dtype=jnp.int32)[None, :]
    adjacency = jnp.where(row_index == col_index, jnp.float32(0.0), powered)
    connectivity = lax.psum(jnp.sum(adjacency, axis=1), "genes")
    return (adjacency, connectivity)


def solution(mesh):
    return jax.shard_map(
        shards,
        mesh=mesh,
        in_specs=(P("cells", "genes"), P("cells")),
        out_specs=(P("cells", "genes"), P("cells")),
        check_vma=False,
    )
```
